32 devices in a mesh: dp: 16 (over z, y, core), sp: 2 (over x).
Axes of the slice: x: 2, y: 2, z: 4, core: 2. Of those that a mesh axis runs over, the one named last changes fastest.
Arguments:
- hidden: bfloat16 [16, 4, 128, 3584], P('dp', None, 'sp'), may hold values from -6 to 6
- segment_ids: int32 [16, 4, 128], P('dp'), may hold values from -1 to 15, as said below
- w_query: bfloat16 [3584, 3584], P(None, 'sp'), may hold values from -0.10022297 to 0.10022297
- key_matrix: bfloat16 [3584, 512], P(None, 'sp'), may hold values from -0.10022297 to 0.10022297
- value_matrix: bfloat16 [3584, 512], P(None, 'sp'), may hold values from -0.10022297 to 0.10022297
Outputs:
- mixed: bfloat16 [16, 512, 3584], P('dp', 'sp')
The draws below stay inside these ranges and needn't reach their ends.
Inputs may be any that keep to these rules, and one draw needn't show every extreme that they name: `segment_ids`: in each outbox the live slots come first; over them the ids start at 0 and never fall, by steps of 0 or 1; empty slots hold -1. Every group has an outbox whose 128 slots are all live.
All inputs are finite; a program needn't handle non-finite values.
Results may differ from the reference program's by a relative error of at most 0.0087.
Values may be sent and summed in bfloat16 or wider, within the bound.
No kernel may reach another device: no remote copies, remote signals or barrier semaphores. Data moves between devices by JAX's collectives and lax.ppermute only.
A program may use at most 64 MiB of HBM per device.

```python
import math
import jax
import jax.numpy as jnp
from jax import lax

MODEL_WIDTH = 3584
QUERY_HEADS = 28
KEY_VALUE_HEADS = 4
HEAD_SIZE = 128
J = 4
B = 128
NSEG = 16
NG = 16
GROUP_SLOTS = 512


def drawn_parts(key):
    key_dir = jax.random.fold_in(key, 21)
    single_key_head = jax.random.fold_in(key, 22)
    direction = jnp.clip(jax.random.normal(key_dir, (MODEL_WIDTH,), jnp.float32), -4.0, 4.0)
    direction = direction / jnp.sqrt(jnp.sum(direction * direction))
    mask_pattern = jnp.clip(jax.random.normal(single_key_head, (KEY_VALUE_HEADS, HEAD_SIZE), jnp.float32), -4.0, 4.0)
    return (direction, mask_pattern)


def draw_w_query(key, part):
    direction, mask_pattern = drawn_parts(key)
    random_noise_key = jax.random.fold_in(key, 31)
    initial_sample = jnp.clip(jax.random.normal(random_noise_key, (MODEL_WIDTH, QUERY_HEADS * HEAD_SIZE), jnp.float32), -5.0, 5.0)
    split_by_head = jnp.repeat(mask_pattern, QUERY_HEADS // KEY_VALUE_HEADS, axis=0).reshape(QUERY_HEADS * HEAD_SIZE)
    weight = initial_sample / math.sqrt(MODEL_WIDTH) + HEAD_SIZE ** (-0.25) * direction[:, None] * split_by_head[None, :]
    bound_value = 6.0 / math.sqrt(MODEL_WIDTH)
    return jnp.clip(weight, -bound_value, bound_value).astype(jnp.bfloat16)


def draw_key_matrix(key, part):
    direction, mask_pattern = drawn_parts(key)
    random_noise_key = jax.random.fold_in(key, 32)
    initial_sample = jnp.clip(jax.random.normal(random_noise_key, (MODEL_WIDTH, KEY_VALUE_HEADS * HEAD_SIZE), jnp.float32), -5.0, 5.0)
    split_by_head = mask_pattern.reshape(KEY_VALUE_HEADS * HEAD_SIZE)
    weight = initial_sample / math.sqrt(MODEL_WIDTH) + HEAD_SIZE ** (-0.25) * direction[:, None] * split_by_head[None, :]
    bound_value = 6.0 / math.sqrt(MODEL_WIDTH)
    return jnp.clip(weight, -bound_value, bound_value).astype(jnp.bfloat16)


def draw_value_matrix(key, part):
    direction = drawn_parts(key)[0]
    random_noise_key = jax.random.fold_in(key, 33)
    initial_sample = jnp.clip(jax.random.normal(random_noise_key, (MODEL_WIDTH, KEY_VALUE_HEADS * HEAD_SIZE), jnp.float32), -5.0, 5.0)
    initial_sample = initial_sample / math.sqrt(MODEL_WIDTH)
    along = jnp.sum(direction[:, None] * initial_sample, axis=0)
    weight = initial_sample - direction[:, None] * along[None, :]
    bound_value = 6.0 / math.sqrt(MODEL_WIDTH)
    return jnp.clip(weight, -bound_value, bound_value).astype(jnp.bfloat16)


def draw_hidden(key, part):
    direction = drawn_parts(key)[0]
    random_noise_key = jax.random.fold_in(key, 41)
    start_key = jax.random.fold_in(key, 42)
    level_key = jax.random.fold_in(key, 43)
    noise_draw = jnp.clip(jax.random.normal(random_noise_key, (NG, J, B, MODEL_WIDTH), jnp.float32), -5.0, 5.0)
    strengths = jnp.array([110.0, 160.0, 220.0, 300.0], jnp.float32)
    run_length = max(B // 8, 2)
    starts = jax.random.randint(start_key, (NG, J), 0, B // 4 - run_length + 1)
    levels = jax.random.randint(level_key, (NG, J), 0, 4)
    picked = (levels[..., None] == jnp.arange(4, dtype=jnp.int32)).astype(jnp.float32)
    amplitude = jnp.sqrt(jnp.sum(picked * strengths, axis=-1))
    slot_index = jnp.arange(B, dtype=jnp.int32)
    inside = (slot_index[None, None, :] >= starts[..., None]) & (slot_index[None, None, :] < starts[..., None] + run_length)
    boost_size = jnp.where(inside, amplitude[..., None], 0.0)
    mixed_rows = noise_draw + boost_size[..., None] * direction
    return jnp.clip(mixed_rows, -6.0, 6.0).astype(jnp.bfloat16)


def draw_segment_ids(key, part):
    key_live = jax.random.fold_in(key, 11)
    key_full = jax.random.fold_in(key, 12)
    key_cuts = jax.random.fold_in(key, 13)
    live_count = jax.random.randint(key_live, (NG, J), B // 4, B + 1)
    full_box = jax.random.randint(key_full, (NG,), 0, J)
    live_count = jnp.where(jnp.arange(J)[None, :] == full_box[:, None], B, live_count)
    index = jnp.arange(B, dtype=jnp.int32)
    cut_marks = (jax.random.randint(key_cuts, (NG, J, B), 0, 12) == 0) & (index[None, None, :] > 0)
    seg_ids = jnp.minimum(jnp.cumsum(cut_marks.astype(jnp.int32), axis=-1), NSEG - 1)
    return jnp.where(index[None, None, :] < live_count[:, :, None], seg_ids, -1).astype(jnp.int32)


def setup_inputs(seed: int = 0) -> dict:
    splits = jax.random.split(jax.random.key(seed), 6)
    hidden = draw_hidden(jax.random.fold_in(splits[5], 71), 0)
    segment_ids = draw_segment_ids(jax.random.fold_in(splits[5], 71), 0)
    w_query = draw_w_query(jax.random.fold_in(splits[5], 71), 0)
    key_matrix = draw_key_matrix(jax.random.fold_in(splits[5], 71), 0)
    value_matrix = draw_value_matrix(jax.random.fold_in(splits[5], 71), 0)
    return dict(hidden=hidden, segment_ids=segment_ids, w_query=w_query, key_matrix=key_matrix, value_matrix=value_matrix)


ROPE_BASE = 1000000.0

def rotate(tensor, where):
    half_width = tensor.shape[-1] // 2
    freq = ROPE_BASE ** (-(jnp.arange(half_width, dtype=jnp.float32) * 2.0 / tensor.shape[-1]))
    angle = where[:, None] * freq[None, :]
    cosine = jnp.cos(angle)[:, None, :]
    sine = jnp.sin(angle)[:, None, :]
    first = tensor[..., :half_width]
    second = tensor[..., half_width:]
    return jnp.concatenate([first * cosine - second * sine, second * cosine + first * sine], axis=-1)

def positions(segments):
    slot_ids = jnp.arange(NSEG, dtype=jnp.int32)
    onehot = (segments[..., :, None] == slot_ids).astype(jnp.int32)
    living = (segments >= 0).astype(jnp.int32)
    below = lax.optimization_barrier(jnp.sum((segments[..., :, None] < slot_ids).astype(jnp.int32) * living[..., :, None], axis=-2))
    first_slot = lax.optimization_barrier(jnp.sum(onehot * below[..., None, :], axis=-1))
    index = jnp.arange(segments.shape[-1], dtype=jnp.int32)
    return (index - first_slot).astype(jnp.float32)

def attend(queries, projected_key_rows, projected_value_rows, labels):
    total_rows = queries.shape[0]
    kv_heads = projected_key_rows.shape[1]
    queries = queries.reshape(total_rows, kv_heads, -1, queries.shape[-1]).astype(jnp.float32)
    scores = jnp.einsum('qcgd,kcd->cgqk', queries, projected_key_rows.astype(jnp.float32)) / jnp.sqrt(jnp.float32(queries.shape[-1]))
    index = jnp.arange(total_rows, dtype=jnp.int32)
    seen = (labels[:, None] == labels[None, :]) & (labels[:, None] >= 0) & (index[None, :] <= index[:, None])
    seen = seen | (index[:, None] == index[None, :])
    scores = jnp.where(seen, scores, -1e+30)
    largest = lax.optimization_barrier(jnp.max(scores, axis=-1, keepdims=True))
    expo = jnp.where(seen, jnp.exp(scores - largest), 0.0)
    denominator = lax.optimization_barrier(jnp.sum(expo, axis=-1, keepdims=True))
    probs = expo.astype(jnp.bfloat16).astype(jnp.float32)
    summed = jnp.einsum('cgqk,kcd->qcgd', probs, projected_value_rows.astype(jnp.float32))
    summed = summed / jnp.transpose(denominator, (2, 0, 1, 3))
    living = (labels >= 0).astype(jnp.float32)
    return (summed.reshape(total_rows, -1) * living[:, None]).astype(jnp.bfloat16)

def reference(hidden, segment_ids, w_query, key_matrix, value_matrix):
    received = jnp.stack([jnp.roll(hidden[:, outbox], outbox, axis=0) for outbox in range(J)], axis=1)
    segments = jnp.stack([jnp.roll(segment_ids[:, outbox], outbox, axis=0) for outbox in range(J)], axis=1)
    where_all = positions(segments)
    box_ids = jnp.arange(J, dtype=jnp.int32)[None, :, None]
    labels = jnp.where(segments >= 0, box_ids * NSEG + segments, -1)

    def one_group(packed):
        slab, where, label_row = packed
        flattened_slots = slab.reshape(GROUP_SLOTS, MODEL_WIDTH)
        where = where.reshape(GROUP_SLOTS)
        queries = jnp.dot(flattened_slots, w_query, preferred_element_type=jnp.float32).reshape(GROUP_SLOTS, QUERY_HEADS, HEAD_SIZE)
        queries = rotate(queries, where).astype(jnp.bfloat16)
        projected_key_rows = jnp.dot(flattened_slots, key_matrix, preferred_element_type=jnp.float32).reshape(GROUP_SLOTS, KEY_VALUE_HEADS, HEAD_SIZE)
        projected_key_rows = rotate(projected_key_rows, where).astype(jnp.bfloat16)
        projected_value_rows = jnp.dot(flattened_slots, value_matrix, preferred_element_type=jnp.float32).astype(jnp.bfloat16).reshape(GROUP_SLOTS, KEY_VALUE_HEADS, HEAD_SIZE)
        return attend(queries, projected_key_rows, projected_value_rows, label_row.reshape(GROUP_SLOTS))
    return lax.map(one_group, (received, where_all, labels))
```

```python
import functools

import jax
import jax.numpy as jnp
from jax import lax
from jax.experimental import pallas as pl
from jax.experimental.pallas import tpu as pltpu
from jax.sharding import PartitionSpec as P

HEAD_SIZE = 128
NSEG = 16
ROPE_BASE = 1000000.0
HIDDEN_SCORE = -1e30


def shifted(value, axis, steps):
    count = lax.axis_size(axis)
    pairs = [(source, (source + steps) % count) for source in range(count)]
    return lax.ppermute(value, axis, pairs)


def positions(segments):
    slot_ids = jnp.arange(NSEG, dtype=jnp.int32)
    onehot = (segments[..., :, None] == slot_ids).astype(jnp.int32)
    living = (segments >= 0).astype(jnp.int32)
    below = jnp.sum(
        (segments[..., :, None] < slot_ids).astype(jnp.int32) * living[..., :, None], axis=-2
    )
    first_slot = jnp.sum(onehot * below[..., None, :], axis=-1)
    index = jnp.arange(segments.shape[-1], dtype=jnp.int32)
    return (index - first_slot).astype(jnp.float32)


def tables(segments):
    where = positions(segments)
    half = HEAD_SIZE // 2
    freq = ROPE_BASE ** (-(jnp.arange(half, dtype=jnp.float32) * 2.0 / HEAD_SIZE))
    angle = where[..., None] * freq
    cosine = jnp.cos(angle)
    sine = jnp.sin(angle)
    cosine = jnp.concatenate([cosine, cosine], axis=-1)
    sine = jnp.concatenate([-sine, sine], axis=-1)
    index = jnp.arange(segments.shape[-1], dtype=jnp.int32)
    row, col = segments[..., :, None], segments[..., None, :]
    seen = (row == col) & (row >= 0) & (index[None, :] <= index[:, None])
    seen = (seen | (index[:, None] == index[None, :])).astype(jnp.float32)
    living = jnp.broadcast_to((row >= 0).astype(jnp.float32), cosine.shape)
    return cosine, sine, seen, living


def box_kernel(parts, place_ref, *refs):
    pieces = refs[:parts]
    cos_ref, sin_ref, seen_ref, live_ref, wq_ref, wk_ref, wv_ref, out_ref, rows = refs[parts:]

    @pl.when(pl.program_id(0) == 0)
    def _():
        size = pieces[0].shape[0]
        for step, piece in enumerate(pieces):
            spot = lax.rem(place_ref[0] - step + parts, parts)
            rows[pl.ds(pl.multiple_of(spot * size, size), size), :] = piece[...]

    cosine, sine = cos_ref[...], sin_ref[...]
    seen = seen_ref[...] > 0.5
    live = live_ref[...]

    def turn(value):
        return (value * cosine + pltpu.roll(value, HEAD_SIZE // 2, 1) * sine).astype(jnp.bfloat16)

    tokens = rows[...]
    keys = turn(jnp.dot(tokens, wk_ref[...], preferred_element_type=jnp.float32))
    values = jnp.dot(tokens, wv_ref[...], preferred_element_type=jnp.float32).astype(jnp.bfloat16)
    queries = jnp.dot(tokens, wq_ref[...], preferred_element_type=jnp.float32)
    root = jnp.sqrt(jnp.float32(HEAD_SIZE))
    for head in range(wq_ref.shape[1] // HEAD_SIZE):
        cols = slice(head * HEAD_SIZE, (head + 1) * HEAD_SIZE)
        query = turn(queries[:, cols])
        scores = lax.dot_general(
            query, keys, (((1,), (1,)), ((), ())), preferred_element_type=jnp.float32
        )
        scores = jnp.where(seen, scores / root, HIDDEN_SCORE)
        expo = jnp.exp(scores - jnp.max(scores, axis=-1, keepdims=True))
        expo = jnp.where(seen, expo, 0.0)
        total = jnp.sum(expo, axis=-1, keepdims=True)
        mixed = jnp.dot(expo.astype(jnp.bfloat16), values, preferred_element_type=jnp.float32)
        out_ref[:, cols] = (mixed / total * live).astype(out_ref.dtype)


def box(place, pieces, table, w_query, key_matrix, value_matrix):
    parts = len(pieces)
    size, width = pieces[0].shape
    slots = parts * size
    kv_heads = key_matrix.shape[1] // HEAD_SIZE
    block = w_query.shape[1] // kv_heads
    whole = lambda c, place: (0, 0)
    mine = lambda c, place: (0, c)
    cols = w_query.shape[1] + 2 * key_matrix.shape[1]
    return pl.pallas_call(
        functools.partial(box_kernel, parts),
        out_shape=jax.ShapeDtypeStruct((slots, w_query.shape[1]), jnp.bfloat16),
        grid_spec=pltpu.PrefetchScalarGridSpec(
            num_scalar_prefetch=1,
            grid=(kv_heads,),
            in_specs=[pl.BlockSpec((size, width), whole)] * parts
            + [pl.BlockSpec((slots, HEAD_SIZE), whole)] * 2
            + [pl.BlockSpec((slots, slots), whole)]
            + [pl.BlockSpec((slots, HEAD_SIZE), whole)]
            + [
                pl.BlockSpec((width, block), mine),
                pl.BlockSpec((width, HEAD_SIZE), mine),
                pl.BlockSpec((width, HEAD_SIZE), mine),
            ],
            out_specs=pl.BlockSpec((slots, block), mine),
            scratch_shapes=[pltpu.VMEM((slots, width), jnp.bfloat16)],
        ),
        compiler_params=pltpu.CompilerParams(vmem_limit_bytes=36 << 20),
        cost_estimate=pl.CostEstimate(
            flops=2 * slots * width * cols,
            bytes_accessed=2 * width * cols + 4 * slots * width,
            transcendentals=slots * w_query.shape[1],
        ),
    )(place, *pieces, *table, w_query, key_matrix, value_matrix)


def join_kernel(parts, place_ref, *refs):
    out_ref = refs[parts]
    width = refs[0].shape[1]
    for step in range(parts):
        spot = lax.rem(place_ref[0] - step + parts, parts)
        out_ref[0, :, pl.ds(pl.multiple_of(spot * width, HEAD_SIZE), width)] = refs[step][...]


def join(place, pieces, held, round_id, rounds):
    parts = len(pieces)
    slots, width = pieces[0].shape
    operands = [place, *pieces]
    in_specs = [pl.BlockSpec((slots, width), lambda i, place: (0, 0))] * parts
    aliases = {}
    kernel = functools.partial(join_kernel, parts)
    if held is not None:
        operands.append(held)
        in_specs.append(pl.BlockSpec(memory_space=pl.ANY))
        aliases = {parts + 1: 0}
        kernel = lambda place_ref, *refs: join_kernel(parts, place_ref, *refs[:parts], refs[parts + 1])
    return pl.pallas_call(
        kernel,
        out_shape=jax.ShapeDtypeStruct((1, rounds * slots, parts * width), jnp.bfloat16),
        grid_spec=pltpu.PrefetchScalarGridSpec(
            num_scalar_prefetch=1,
            grid=(1,),
            in_specs=in_specs,
            out_specs=pl.BlockSpec((1, slots, parts * width), lambda i, place: (0, round_id, 0)),
        ),
        input_output_aliases=aliases,
        compiler_params=pltpu.CompilerParams(vmem_limit_bytes=16 << 20),
        cost_estimate=pl.CostEstimate(
            flops=0, bytes_accessed=4 * slots * parts * width, transcendentals=0
        ),
    )(*operands)


def local(hidden, segment_ids, w_query, key_matrix, value_matrix):
    outboxes = hidden.shape[1]
    parts = lax.axis_size("sp")
    rounds = outboxes // parts
    place = lax.axis_index("sp").astype(jnp.int32)
    place_arg = place[None]
    labels = [segment_ids[0, 0]] + [
        shifted(segment_ids[0, stride], "dp", stride) for stride in range(1, outboxes)
    ]
    tokens = [hidden[0, 0]] + [
        shifted(hidden[0, stride], "dp", stride) for stride in range(1, outboxes)
    ]
    table = tables(jnp.stack(labels))
    results = []
    for number in range(outboxes):
        pieces = [tokens[number]] + [
            shifted(tokens[number], "sp", step) for step in range(1, parts)
        ]
        results.append(
            box(place_arg, pieces, [t[number] for t in table], w_query, key_matrix, value_matrix)
        )
    held = None
    for turn in range(rounds):
        group = [results[owner * rounds + turn] for owner in range(parts)]
        pieces = []
        for step in range(parts):
            target = lax.rem(place + step, parts)
            chosen = lax.select_n(target, *group) if parts > 2 else (
                jnp.where(target == 0, group[0], group[-1])
            )
            pieces.append(chosen if step == 0 else shifted(chosen, "sp", step))
        held = join(place_arg, pieces, held, turn, rounds)
    return held


def solution(mesh):
    placed = (
        P("dp", None, "sp", None),
        P("dp", None, None),
        P(None, "sp"),
        P(None, "sp"),
        P(None, "sp"),
    )
    return jax.shard_map(
        local, mesh=mesh, in_specs=placed, out_specs=P("dp", "sp", None), check_vma=False
    )
```

```python
import functools

import jax
import jax.numpy as jnp
from jax import lax
from jax.experimental import pallas as pl
from jax.experimental.pallas import tpu as pltpu
from jax.sharding import PartitionSpec as P


HEAD_SIZE = 128
NSEG = 16
ROPE_BASE = 1000000.0
HIDDEN_SCORE = -1e30


def shifted(value, axis, steps):
    count = lax.axis_size(axis)
    pairs = [(source, (source + steps) % count) for source in range(count)]
    return lax.ppermute(value, axis, pairs)


def positions(segments):
    slot_ids = jnp.arange(NSEG, dtype=jnp.int32)
    onehot = (segments[..., :, None] == slot_ids).astype(jnp.int32)
    living = (segments >= 0).astype(jnp.int32)
    below = jnp.sum(
        (segments[..., :, None] < slot_ids).astype(jnp.int32) * living[..., :, None], axis=-2
    )
    first_slot = jnp.sum(onehot * below[..., None, :], axis=-1)
    index = jnp.arange(segments.shape[-1], dtype=jnp.int32)
    return (index - first_slot).astype(jnp.float32)


def tables(segments):
    where = positions(segments)
    half = HEAD_SIZE // 2
    freq = ROPE_BASE ** (-(jnp.arange(half, dtype=jnp.float32) * 2.0 / HEAD_SIZE))
    angle = where[..., None] * freq
    cosine = jnp.cos(angle)
    sine = jnp.sin(angle)
    cosine = jnp.concatenate([cosine, cosine], axis=-1)
    sine = jnp.concatenate([-sine, sine], axis=-1)
    index = jnp.arange(segments.shape[-1], dtype=jnp.int32)
    row, col = segments[..., :, None], segments[..., None, :]
    seen = (row == col) & (row >= 0) & (index[None, :] <= index[:, None])
    seen = (seen | (index[:, None] == index[None, :])).astype(jnp.float32)
    living = jnp.broadcast_to((row >= 0).astype(jnp.float32), cosine.shape)
    return cosine, sine, seen, living


def box_kernel(parts, place_ref, *refs):
    pieces = refs[:parts]
    cos_ref, sin_ref, seen_ref, live_ref, wq_ref, wk_ref, wv_ref, out_ref, rows = refs[parts:]

    @pl.when(pl.program_id(0) == 0)
    def _():
        size = pieces[0].shape[0]
        for step, piece in enumerate(pieces):
            spot = lax.rem(place_ref[0] - step + parts, parts)
            rows[pl.ds(pl.multiple_of(spot * size, size), size), :] = piece[...]

    cosine, sine = cos_ref[...], sin_ref[...]
    seen = seen_ref[...] > 0.5
    live = live_ref[...]

    def turn(value):
        return (value * cosine + pltpu.roll(value, HEAD_SIZE // 2, 1) * sine).astype(jnp.bfloat16)

    tokens = rows[...]
    keys = turn(jnp.dot(tokens, wk_ref[...], preferred_element_type=jnp.float32))
    values = jnp.dot(tokens, wv_ref[...], preferred_element_type=jnp.float32).astype(jnp.bfloat16)
    queries = jnp.dot(tokens, wq_ref[...], preferred_element_type=jnp.float32)
    root = jnp.sqrt(jnp.float32(HEAD_SIZE))
    for head in range(wq_ref.shape[1] // HEAD_SIZE):
        cols = slice(head * HEAD_SIZE, (head + 1) * HEAD_SIZE)
        query = turn(queries[:, cols])
        scores = lax.dot_general(
            query, keys, (((1,), (1,)), ((), ())), preferred_element_type=jnp.float32
        )
        scores = jnp.where(seen, scores / root, HIDDEN_SCORE)
        expo = jnp.exp(scores - jnp.max(scores, axis=-1, keepdims=True))
        expo = jnp.where(seen, expo, 0.0)
        total = jnp.sum(expo, axis=-1, keepdims=True)
        mixed = jnp.dot(expo.astype(jnp.bfloat16), values, preferred_element_type=jnp.float32)
        out_ref[:, cols] = (mixed / total * live).astype(out_ref.dtype)


def box(place, pieces, table, w_query, key_matrix, value_matrix):
    parts = len(pieces)
    size, width = pieces[0].shape
    slots = parts * size
    kv_heads = key_matrix.shape[1] // HEAD_SIZE
    block = w_query.shape[1] // kv_heads
    whole = lambda c, place: (0, 0)
    mine = lambda c, place: (0, c)
    cols = w_query.shape[1] + 2 * key_matrix.shape[1]
    return pl.pallas_call(
        functools.partial(box_kernel, parts),
        out_shape=jax.ShapeDtypeStruct((slots, w_query.shape[1]), jnp.bfloat16),
        grid_spec=pltpu.PrefetchScalarGridSpec(
            num_scalar_prefetch=1,
            grid=(kv_heads,),
            in_specs=[pl.BlockSpec((size, width), whole)] * parts
            + [pl.BlockSpec((slots, HEAD_SIZE), whole)] * 2
            + [pl.BlockSpec((slots, slots), whole)]
            + [pl.BlockSpec((slots, HEAD_SIZE), whole)]
            + [
                pl.BlockSpec((width, block), mine),
                pl.BlockSpec((width, HEAD_SIZE), mine),
                pl.BlockSpec((width, HEAD_SIZE), mine),
            ],
            out_specs=pl.BlockSpec((slots, block), mine),
            scratch_shapes=[pltpu.VMEM((slots, width), jnp.bfloat16)],
        ),
        compiler_params=pltpu.CompilerParams(vmem_limit_bytes=54 << 20),
        cost_estimate=pl.CostEstimate(
            flops=2 * slots * width * cols,
            bytes_accessed=2 * width * cols + 4 * slots * width,
            transcendentals=slots * w_query.shape[1],
        ),
    )(place, *pieces, *table, w_query, key_matrix, value_matrix)


def join_kernel(parts, place_ref, *refs):
    out_ref = refs[parts]
    width = refs[0].shape[1]
    for step in range(parts):
        spot = lax.rem(place_ref[0] - step + parts, parts)
        out_ref[0, :, pl.ds(pl.multiple_of(spot * width, HEAD_SIZE), width)] = refs[step][...]


def join(place, pieces, held, round_id, rounds):
    parts = len(pieces)
    slots, width = pieces[0].shape
    operands = [place, *pieces]
    in_specs = [pl.BlockSpec((slots, width), lambda i, place: (0, 0))] * parts
    aliases = {}
    kernel = functools.partial(join_kernel, parts)
    if held is not None:
        operands.append(held)
        in_specs.append(pl.BlockSpec(memory_space=pl.ANY))
        aliases = {parts + 1: 0}
        kernel = lambda place_ref, *refs: join_kernel(parts, place_ref, *refs[:parts], refs[parts + 1])
    return pl.pallas_call(
        kernel,
        out_shape=jax.ShapeDtypeStruct((1, rounds * slots, parts * width), jnp.bfloat16),
        grid_spec=pltpu.PrefetchScalarGridSpec(
            num_scalar_prefetch=1,
            grid=(1,),
            in_specs=in_specs,
            out_specs=pl.BlockSpec((1, slots, parts * width), lambda i, place: (0, round_id, 0)),
        ),
        input_output_aliases=aliases,
        compiler_params=pltpu.CompilerParams(vmem_limit_bytes=16 << 20),
        cost_estimate=pl.CostEstimate(
            flops=0, bytes_accessed=4 * slots * parts * width, transcendentals=0
        ),
    )(*operands)


def plan(outboxes):
    late = [number for number in range(outboxes) if number % 2]
    order = late[::-1] + [number for number in range(outboxes) if number not in late]
    return order, [number if number in late else 0 for number in range(outboxes)]


def sent_home(value, step, targets):
    groups, parts = lax.axis_size("dp"), lax.axis_size("sp")
    pairs = []
    for group in range(groups):
        for place in range(parts):
            target = (place + step) % parts
            pairs.append(
                (group * parts + place, (group + targets[target]) % groups * parts + target)
            )
    return lax.ppermute(value, ("dp", "sp"), pairs)


def local(hidden, segment_ids, w_query, key_matrix, value_matrix):
    outboxes = hidden.shape[1]
    parts = lax.axis_size("sp")
    rounds = outboxes // parts
    place = lax.axis_index("sp").astype(jnp.int32)
    place_arg = place[None]
    order, moves = plan(outboxes)
    tokens, labels = {}, {}
    for number in order:
        stride = number - moves[number]
        token, label = hidden[0, number], segment_ids[0, number]
        if stride:
            label = shifted(label, "dp", stride)
            token = shifted(token, "dp", stride)
        tokens[number], labels[number] = token, label
    table = tables(jnp.stack([labels[number] for number in range(outboxes)]))
    results = {}
    for number in order:
        pieces = [tokens[number]] + [
            shifted(tokens[number], "sp", step) for step in range(1, parts)
        ]
        results[number] = box(
            place_arg, pieces, [t[number] for t in table], w_query, key_matrix, value_matrix
        )
    held = None
    for turn in reversed(range(rounds)):
        members = [owner * rounds + turn for owner in range(parts)]
        group = [results[number] for number in members]
        targets = [moves[number] for number in members]
        pieces = []
        for step in range(parts):
            target = lax.rem(place + step, parts)
            chosen = lax.select_n(target, *group) if parts > 2 else (
                jnp.where(target == 0, group[0], group[-1])
            )
            if step or any(targets):
                chosen = sent_home(chosen, step, targets)
            pieces.append(chosen)
        held = join(place_arg, pieces, held, turn, rounds)
    return held


def solution(mesh):
    placed = (
        P("dp", None, "sp", None),
        P("dp", None, None),
        P(None, "sp"),
        P(None, "sp"),
        P(None, "sp"),
    )

    return jax.shard_map(
        local, mesh=mesh, in_specs=placed, out_specs=P("dp", "sp", None), check_vma=False
    )
```

```python
import functools

import jax
import jax.numpy as jnp
from jax import lax
from jax.experimental import pallas as pl
from jax.experimental.pallas import tpu as pltpu
from jax.sharding import PartitionSpec as P


HEAD_SIZE = 128
NSEG = 16
ROPE_BASE = 1000000.0
HIDDEN_SCORE = -1e30


def shifted(value, axis, steps):
    count = lax.axis_size(axis)
    pairs = [(source, (source + steps) % count) for source in range(count)]
    return lax.ppermute(value, axis, pairs)


def positions(segments):
    slot_ids = jnp.arange(NSEG, dtype=jnp.int32)
    onehot = (segments[..., :, None] == slot_ids).astype(jnp.int32)
    living = (segments >= 0).astype(jnp.int32)
    below = jnp.sum(
        (segments[..., :, None] < slot_ids).astype(jnp.int32) * living[..., :, None], axis=-2
    )
    first_slot = jnp.sum(onehot * below[..., None, :], axis=-1)
    index = jnp.arange(segments.shape[-1], dtype=jnp.int32)
    return (index - first_slot).astype(jnp.float32)


def tables(segments):
    where = positions(segments)
    half = HEAD_SIZE // 2
    freq = ROPE_BASE ** (-(jnp.arange(half, dtype=jnp.float32) * 2.0 / HEAD_SIZE))
    angle = where[..., None] * freq
    cosine = jnp.cos(angle)
    sine = jnp.sin(angle)
    cosine = jnp.concatenate([cosine, cosine], axis=-1)
    sine = jnp.concatenate([-sine, sine], axis=-1)
    index = jnp.arange(segments.shape[-1], dtype=jnp.int32)
    row, col = segments[..., :, None], segments[..., None, :]
    seen = (row == col) & (row >= 0) & (index[None, :] <= index[:, None])
    seen = seen | (index[:, None] == index[None, :])
    bias = jnp.where(seen, 0.0, HIDDEN_SCORE).astype(jnp.float32)
    living = jnp.broadcast_to((row >= 0).astype(jnp.float32), cosine.shape)
    return cosine, sine, bias, living


def box_kernel(parts, place_ref, *refs):
    pieces = refs[:parts]
    cos_ref, sin_ref, seen_ref, live_ref, wq_ref, wk_ref, wv_ref, out_ref, rows = refs[parts:]

    @pl.when(pl.program_id(0) == 0)
    def _():
        size = pieces[0].shape[0]
        for step, piece in enumerate(pieces):
            spot = lax.rem(place_ref[0] - step + parts, parts)
            rows[pl.ds(pl.multiple_of(spot * size, size), size), :] = piece[...]

    cosine, sine, bias = cos_ref[0], sin_ref[0], seen_ref[0]
    live = live_ref[0][:, :1]

    def turn(value):
        return (value * cosine + pltpu.roll(value, HEAD_SIZE // 2, 1) * sine).astype(jnp.bfloat16)

    tokens = rows[...]
    keys = turn(jnp.dot(tokens, wk_ref[...], preferred_element_type=jnp.float32))
    queries = jnp.dot(tokens, wq_ref[...], preferred_element_type=jnp.float32)
    values = jnp.dot(tokens, wv_ref[...], preferred_element_type=jnp.float32).astype(jnp.bfloat16)
    spans = [
        slice(head * HEAD_SIZE, (head + 1) * HEAD_SIZE)
        for head in range(wq_ref.shape[1] // HEAD_SIZE)
    ]
    turned = [turn(queries[:, span]) for span in spans]
    scores = [
        lax.dot_general(query, keys, (((1,), (1,)), ((), ())), preferred_element_type=jnp.float32)
        for query in turned
    ]
    scores = [score * (HEAD_SIZE ** -0.5) + bias for score in scores]
    tops = [jnp.max(score, axis=-1, keepdims=True) for score in scores]
    expos = [jnp.exp(score - top) for score, top in zip(scores, tops)]
    factors = [live / jnp.sum(expo, axis=-1, keepdims=True) for expo in expos]
    mixes = [
        jnp.dot(expo.astype(jnp.bfloat16), values, preferred_element_type=jnp.float32)
        for expo in expos
    ]
    for span, mixed, factor in zip(spans, mixes, factors):
        out_ref[:, span] = (mixed * factor).astype(out_ref.dtype)


def box(place, number, pieces, table, w_query, key_matrix, value_matrix):
    parts = len(pieces)
    size, width = pieces[0].shape
    slots = parts * size
    kv_heads = key_matrix.shape[1] // HEAD_SIZE
    block = w_query.shape[1] // kv_heads
    whole = lambda c, place: (0, 0)
    mine = lambda c, place: (0, c)
    ours = lambda c, place: (number, 0, 0)
    cols = w_query.shape[1] + 2 * key_matrix.shape[1]
    return pl.pallas_call(
        functools.partial(box_kernel, parts),
        out_shape=jax.ShapeDtypeStruct((slots, w_query.shape[1]), jnp.bfloat16),
        grid_spec=pltpu.PrefetchScalarGridSpec(
            num_scalar_prefetch=1,
            grid=(kv_heads,),
            in_specs=[pl.BlockSpec((size, width), whole)] * parts
            + [pl.BlockSpec((1,) + entry.shape[1:], ours) for entry in table]
            + [
                pl.BlockSpec((width, block), mine),
                pl.BlockSpec((width, HEAD_SIZE), mine),
                pl.BlockSpec((width, HEAD_SIZE), mine),
            ],
            out_specs=pl.BlockSpec((slots, block), mine),
            scratch_shapes=[pltpu.VMEM((slots, width), jnp.bfloat16)],
        ),
        compiler_params=pltpu.CompilerParams(vmem_limit_bytes=52 << 20),
        cost_estimate=pl.CostEstimate(
            flops=2 * slots * width * cols,
            bytes_accessed=2 * width * cols + 4 * slots * width,
            transcendentals=slots * w_query.shape[1],
        ),
    )(place, *pieces, *table, w_query, key_matrix, value_matrix)


def join_kernel(parts, place_ref, *refs):
    out_ref = refs[parts]
    width = refs[0].shape[1]
    for step in range(parts):
        spot = lax.rem(place_ref[0] - step + parts, parts)
        out_ref[0, :, pl.ds(pl.multiple_of(spot * width, HEAD_SIZE), width)] = refs[step][...]


def join(place, pieces, held, round_id, rounds):
    parts = len(pieces)
    slots, width = pieces[0].shape
    operands = [place, *pieces]
    in_specs = [pl.BlockSpec((slots, width), lambda i, place: (0, 0))] * parts
    aliases = {}
    kernel = functools.partial(join_kernel, parts)
    if held is not None:
        operands.append(held)
        in_specs.append(pl.BlockSpec(memory_space=pl.ANY))
        aliases = {parts + 1: 0}
        kernel = lambda place_ref, *refs: join_kernel(
            parts, place_ref, *refs[:parts], refs[parts + 1]
        )
    return pl.pallas_call(
        kernel,
        out_shape=jax.ShapeDtypeStruct((1, rounds * slots, parts * width), jnp.bfloat16),
        grid_spec=pltpu.PrefetchScalarGridSpec(
            num_scalar_prefetch=1,
            grid=(1,),
            in_specs=in_specs,
            out_specs=pl.BlockSpec((1, slots, parts * width), lambda i, place: (0, round_id, 0)),
        ),
        input_output_aliases=aliases,
        compiler_params=pltpu.CompilerParams(vmem_limit_bytes=16 << 20),
        cost_estimate=pl.CostEstimate(
            flops=0, bytes_accessed=4 * slots * parts * width, transcendentals=0
        ),
    )(*operands)


def plan(outboxes):
    late = [number for number in range(outboxes) if number % 2]
    order = late[::-1] + [number for number in range(outboxes) if number not in late]
    return order, [number if number in late else 0 for number in range(outboxes)]


def sent_home(value, step, targets):
    groups, parts = lax.axis_size("dp"), lax.axis_size("sp")
    pairs = []
    for group in range(groups):
        for place in range(parts):
            target = (place + step) % parts
            pairs.append(
                (group * parts + place, (group + targets[target]) % groups * parts + target)
            )
    return lax.ppermute(value, ("dp", "sp"), pairs)


def local(hidden, segment_ids, w_query, key_matrix, value_matrix):
    outboxes = hidden.shape[1]
    parts = lax.axis_size("sp")
    rounds = outboxes // parts
    place = lax.axis_index("sp").astype(jnp.int32)
    place_arg = place[None]
    order, moves = plan(outboxes)
    tokens, labels = {}, {}
    for number in order:
        stride = number - moves[number]
        token, label = hidden[0, number], segment_ids[0, number]
        if stride:
            label = shifted(label, "dp", stride)
            token = shifted(token, "dp", stride)
        tokens[number], labels[number] = token, label
    table = tables(jnp.stack([labels[number] for number in range(outboxes)]))
    results = {}
    for number in order:
        pieces = [tokens[number]] + [
            shifted(tokens[number], "sp", step) for step in range(1, parts)
        ]
        results[number] = box(place_arg, number, pieces, table, w_query, key_matrix, value_matrix)
    held = None
    for turn in reversed(range(rounds)):
        members = [owner * rounds + turn for owner in range(parts)]
        group = [results[number] for number in members]
        targets = [moves[number] for number in members]
        pieces = []
        for step in range(parts):
            target = lax.rem(place + step, parts)
            chosen = lax.select_n(target, *group) if parts > 2 else (
                jnp.where(target == 0, group[0], group[-1])
            )
            if step or any(targets):
                chosen = sent_home(chosen, step, targets)
            pieces.append(chosen)
        held = join(place_arg, pieces, held, turn, rounds)
    return held


def solution(mesh):
    placed = (
        P("dp", None, "sp", None),
        P("dp", None, None),
        P(None, "sp"),
        P(None, "sp"),
        P(None, "sp"),
    )

    return jax.shard_map(
        local, mesh=mesh, in_specs=placed, out_specs=P("dp", "sp", None), check_vma=False
    )
```
